32 devices in a mesh: rep: 2 (over x), dp: 16 (over y, z, core).
Axes of the slice: x: 2, y: 2, z: 4, core: 2. Of those that a mesh axis runs over, the one named last changes fastest.
Arguments:
- x: bfloat16 [32, 2048, 1024], P(('rep', 'dp')), parts along dimension 0
- dy: bfloat16 [32, 2048, 1024], P(('rep', 'dp')), parts along dimension 0
- w_gate: bfloat16 [2, 1024, 2816], replicated
- w_up: bfloat16 [2, 1024, 2816], replicated
- w_down: bfloat16 [2, 2816, 1024], replicated
- m_w_gate: float32 [2, 1024, 2816], P(None, 'dp')
- m_w_up: float32 [2, 1024, 2816], P(None, 'dp')
- m_w_down: float32 [2, 2816, 1024], P(None, 'dp')
- v_w_gate: float32 [2, 1024, 2816], P(None, 'dp')
- v_w_up: float32 [2, 1024, 2816], P(None, 'dp')
- v_w_down: float32 [2, 2816, 1024], P(None, 'dp')
Outputs:
- output 1: bfloat16 [4, 1024, 2816], P('rep'), parts along dimension 0
- output 2: bfloat16 [4, 1024, 2816], P('rep'), parts along dimension 0
- output 3: bfloat16 [4, 2816, 1024], P('rep'), parts along dimension 0
- output 4: float32 [4, 1024, 2816], P('rep', 'dp'), parts along dimension 0
- output 5: float32 [4, 1024, 2816], P('rep', 'dp'), parts along dimension 0
- output 6: float32 [4, 2816, 1024], P('rep', 'dp'), parts along dimension 0
- output 7: float32 [4, 1024, 2816], P('rep', 'dp'), parts along dimension 0
- output 8: float32 [4, 1024, 2816], P('rep', 'dp'), parts along dimension 0
- output 9: float32 [4, 2816, 1024], P('rep', 'dp'), parts along dimension 0
There are 2 independent parts. The reference program is written for one: setup_inputs(seed, part) draws one part's arguments, and reference() takes and returns one part's arrays. A program takes and returns all parts, laid end to end along the dimension named above; an argument that names none is the same for every part.
All inputs are finite; a program needn't handle non-finite values.
Results may differ from the reference program's by a relative error of at most 0.02.
Values are sent between devices in bfloat16 or wider.
A program may use at most 2 GiB of HBM per device.

```python
import jax
import jax.numpy as jnp
from jax import lax

SEQUENCES = 16
TOKENS = 2048
D = 1024
FF = 2816
LAYERS = 2
NAMES = ("w_gate", "w_up", "w_down")
SHAPES = {"w_gate": (LAYERS, D, FF), "w_up": (LAYERS, D, FF), "w_down": (LAYERS, FF, D)}


def bump(key, n, height):
    away = (jnp.arange(n, dtype=jnp.int32) - jax.random.randint(key, (), 0, n, jnp.int32)) % n
    return jnp.where(away < n // 8, height, 1.0)


def together(key, own, strength):
    shared = jax.random.normal(key, own.shape[1:], jnp.float32)
    return (own + strength * shared) * lax.rsqrt(1 + strength * strength)


def setup_inputs(seed: int = 0, part: int = 0) -> dict:
    kx, kdy, ka, kb, kz, kf, kh, kl, *keys = jax.random.split(jax.random.key(seed), 8 + 3 * len(NAMES))
    kx, kdy, ka, kb = (jax.random.fold_in(k, part) for k in (kx, kdy, ka, kb))
    kw, km, kv = (keys[i::3] for i in range(3))
    shape = (SEQUENCES, TOKENS, D)
    much_x, much_dy = jax.random.uniform(kz, (2,), jnp.float32, 0.0, 1.0)
    loud = 2.0 ** jax.random.uniform(jax.random.fold_in(kz, 1), (), jnp.float32, -1.0, 2.0)
    layers = 2.0 ** jax.random.uniform(kl, (LAYERS, 1, 1), jnp.float32, -1.0, 1.0)
    x = together(ka, jax.random.normal(kx, shape, jnp.float32), much_x) * bump(kf, D, 4.0)
    dy = together(kb, jax.random.normal(kdy, shape, jnp.float32), much_dy)
    drawn = {"x": x.astype(jnp.bfloat16), "dy": (loud * dy * (SEQUENCES * TOKENS) ** -0.5).astype(jnp.bfloat16)}
    for key, name in zip(kw, NAMES, strict=True):
        w = jax.random.normal(key, SHAPES[name], jnp.float32) * SHAPES[name][1] ** -0.5
        drawn[name] = (w * {"w_gate": 1.0, "w_up": bump(kh, FF, 4.0), "w_down": layers}[name]).astype(jnp.bfloat16)
    for key, name in zip(km, NAMES, strict=True):
        drawn[f"m_{name}"] = 0.1 * jax.random.normal(key, SHAPES[name], jnp.float32)
    for key, name in zip(kv, NAMES, strict=True):
        drawn[f"v_{name}"] = jax.random.uniform(key, SHAPES[name], jnp.float32, 0.005, 0.015)
    return drawn


def matmul(a, w):
    return jnp.dot(a, w, preferred_element_type=jnp.float32).astype(jnp.bfloat16)


def normed(h):
    wide = h.astype(jnp.float32)
    scale = lax.rsqrt(jnp.mean(wide**2, -1, keepdims=True) + 1e-6)
    return (wide * scale).astype(jnp.bfloat16)


def layer(h, w):
    a = normed(h)
    gate = jnp.dot(a, w["w_gate"], preferred_element_type=jnp.float32)
    up = jnp.dot(a, w["w_up"], preferred_element_type=jnp.float32)
    return h + matmul((jax.nn.silu(gate) * up).astype(jnp.bfloat16), w["w_down"])


def adamw(w, m, v, g):
    m = 0.9 * m + 0.1 * g
    v = 0.95 * v + 0.05 * g * g
    step = m * lax.rsqrt(v + 1e-8) + 0.1 * w
    return (w - 0.02 * step).astype(jnp.bfloat16), m, v


def stack(weights, h):
    return lax.scan(lambda h, w: (layer(h, w), None), h, weights)[0]


def reference(x, dy, w_gate, w_up, w_down, m_w_gate, m_w_up, m_w_down, v_w_gate, v_w_up, v_w_down):
    weights = dict(zip(NAMES, (w_gate, w_up, w_down), strict=True))

    def take(so_far, sequence):
        h, by_y = sequence
        _, back = jax.vjp(lambda w: stack(w, h), weights)
        return jax.tree.map(lambda total, term: total + term.astype(jnp.float32), so_far, back(by_y)[0]), None

    none_yet = {name: jnp.zeros(w.shape, jnp.float32) for name, w in weights.items()}
    by_weights, _ = lax.scan(take, none_yet, (x, dy))
    gradients = [by_weights[name].astype(jnp.bfloat16).astype(jnp.float32) for name in NAMES]
    new = [
        adamw(w.astype(jnp.float32), m, v, g)
        for w, m, v, g in zip((w_gate, w_up, w_down), (m_w_gate, m_w_up, m_w_down), (v_w_gate, v_w_up, v_w_down), gradients, strict=True)
    ]
    return tuple(one[which] for which in range(3) for one in new)
```

```python
import functools

import jax
import jax.numpy as jnp
from jax import lax
from jax.experimental import pallas as pl
from jax.experimental.pallas import tpu as pltpu
from jax.sharding import PartitionSpec as P

F32, BF16 = jnp.float32, jnp.bfloat16
KINDS = 3
CHUNK = 256


def matmul(a, w):
    return jnp.dot(a, w, preferred_element_type=F32).astype(BF16)


def matmul_t(a, w):
    return lax.dot_general(a, w, (((1,), (1,)), ((), ())), preferred_element_type=F32).astype(BF16)


def inverse_rms(h):
    wide = h.astype(F32)
    return lax.rsqrt(jnp.mean(wide**2, -1, keepdims=True) + 1e-6)


def forward(h, wg, wu):
    scale = inverse_rms(h)
    a = (h.astype(F32) * scale).astype(BF16)
    gate = jnp.dot(a, wg, preferred_element_type=F32)
    up = jnp.dot(a, wu, preferred_element_type=F32)
    act = (jax.nn.silu(gate) * up).astype(BF16)
    return a, gate, up, act


def through_product(gate, up, dact):
    dact = dact.astype(F32)
    s = jax.nn.sigmoid(gate)
    silu = gate * s
    dgate = dact * up * (s + silu * (1 - s))
    return dgate.astype(BF16), (dact * silu).astype(BF16)


def through_norm(h, da):
    wide, da = h.astype(F32), da.astype(F32)
    scale = inverse_rms(h)
    inner = jnp.sum(da * wide, -1, keepdims=True)
    return (da * scale - wide * (scale**3 * inner / h.shape[-1])).astype(BF16)


def chain(x, dy, wg, wu, wd):
    a0, gate0, up0, act0 = forward(x, wg[0], wu[0])
    h1 = x + matmul(act0, wd[0])
    a1, gate1, up1, act1 = forward(h1, wg[1], wu[1])
    dgate1, dup1 = through_product(gate1, up1, matmul_t(dy, wd[1]))
    da = matmul_t(dgate1, wg[1]) + matmul_t(dup1, wu[1])
    dh0 = dy + through_norm(h1, da)
    dgate0, dup0 = through_product(gate0, up0, matmul_t(dh0, wd[0]))
    return (a0, dgate0, dup0, act0, dh0), (a1, dgate1, dup1, act1, dy)


def tail_kernel(ny, nz, units, *refs):
    layers = 2
    acts = [refs[5 * n : 5 * n + 5] for n in range(layers)]
    refs = refs[5 * layers :]
    ws, ms, vs, nws, nms, nvs = (refs[3 * i : 3 * i + 3] for i in range(6))
    zrecv = refs[18:20]
    (g0, g1, c0, c1, y0, y1, cs0, cs1, mst0, mst1, vst0, vst1, wst0, wst1, zst0, zst1, at, ach, bt,
     c_s, c_r, y_s, y_r, z_s, z_r, agz_s, agz_r, agy_s, agy_r, agc_s, agc_r, asem, bsem, lsem, osem) = refs[20:]
    G, C, Y, CS = (g0, g1), (c0, c1), (y0, y1), (cs0, cs1)
    MST, VST, WST, ZST = (mst0, mst1), (vst0, vst1), (wst0, wst1), (zst0, zst1)

    me = lax.axis_index("dp")
    c = lax.rem(me, 2)
    z = lax.rem(lax.div(me, 2), nz)
    y = lax.div(me, 2 * nz)

    def at_(yy, zz, cc):
        return (yy * nz + zz) * 2 + cc

    def zrel(k):
        return lax.rem(z + k + nz, nz)

    core_peer = at_(y, z, 1 - c)
    y_peer = at_(1 - y, z, c)
    z_peers = [at_(y, zrel(k), c) for k in range(1, nz)]

    def remote(src, dst, ss, rs, dev):
        return pltpu.make_async_remote_copy(
            src_ref=src, dst_ref=dst, send_sem=ss, recv_sem=rs, device_id={"dp": dev}, device_id_type=pl.DeviceIdType.MESH
        )

    barrier = pltpu.get_barrier_semaphore()
    for dev in [core_peer, y_peer, *z_peers]:
        pl.semaphore_signal(barrier, inc=1, device_id={"dp": dev}, device_id_type=pl.DeviceIdType.MESH)
    pl.semaphore_wait(barrier, 2 + len(z_peers))

    info = []
    seen = [0, 0]
    for layer, kind in units:
        t = int(kind == 2)
        info.append((layer, kind, t, seen[t]))
        seen[t] += 1

    def rows_of(t):
        return G[t].shape[3], G[t].shape[4]

    def c_copy(u, h):
        layer, kind, t, i = info[u]
        return remote(CS[t], C[t].at[i, h], c_s.at[u, h], c_r.at[u, h], core_peer)

    def y_copy(u, j):
        layer, kind, t, i = info[u]
        zz = zrel(j)
        return remote(G[t].at[i, 0, zz], Y[t].at[i, zz], y_s.at[u, j], y_r.at[u, j], y_peer)

    def z_copy(u, k):
        layer, kind, t, i = info[u]
        return remote(G[t].at[i, 1, zrel(k)], zrecv[t].at[i, k - 1], z_s.at[u, k - 1], z_r.at[u, k - 1], z_peers[k - 1])

    def spot(u, d):
        layer, kind, t, i = info[u]
        rows = rows_of(t)[0]
        return nws[kind].at[layer, pl.ds(pl.multiple_of(d * rows, rows), rows), :]

    last_c = [None, None]

    def compute(u, h):
        layer, kind, t, i = info[u]
        a, dgate, dup, act, dh = acts[layer]
        lhs, rhs = ((a, dgate), (a, dup), (act, dh))[kind]
        rows, cols = rows_of(t)
        tokens = lhs.shape[0]
        half = nz * 2 * rows
        yy = y if h else 1 - y
        steps, tiles = tokens // CHUNK, cols // CHUNK

        def get_a(s):
            where = pl.ds(pl.multiple_of(s * CHUNK, CHUNK), CHUNK)
            return pltpu.make_async_copy(lhs.at[where, pl.ds(pl.multiple_of(yy * half, 128), half)], at.at[where, :half], asem.at[0])

        def get_b(n, slot):
            return pltpu.make_async_copy(rhs.at[:, pl.ds(pl.multiple_of(n * CHUNK, CHUNK), CHUNK)], bt.at[slot], bsem.at[slot])

        whole = pltpu.make_async_copy(lhs.at[:, pl.ds(pl.multiple_of(yy * half, 128), half)], at.at[:, :half], asem.at[0])
        whole.start()
        get_b(0, 0).start()

        whole.wait()
        if last_c[t] is not None:
            c_copy(*last_c[t]).wait_send()

        @pl.loop(0, tiles)
        def _(n):
            slot = lax.rem(n, 2)

            @pl.when(n + 1 < tiles)
            def _():
                get_b(n + 1, 1 - slot).start()

            get_b(n, slot).wait()
            out = lax.dot_general(at[:, :half], bt[slot], (((0,), (0,)), ((), ())), preferred_element_type=F32).astype(BF16)
            out = out.reshape(nz, 2, rows, CHUNK)
            where = pl.ds(pl.multiple_of(n * CHUNK, CHUNK), CHUNK)
            for zz in range(nz):
                first, second = out[zz, 0], out[zz, 1]
                G[t][i, h, zz, :, where] = jnp.where(c == 0, first, second)
                CS[t][zz, :, where] = jnp.where(c == 0, second, first)

        c_copy(u, h).start()
        last_c[t] = (u, h)

    def pieces(t, body):
        rows, cols = rows_of(t)
        wide = cols // 2 if cols > 2048 else cols

        @pl.loop(0, rows // 16)
        def _(r):
            for n in range(0, cols, wide):
                body(pl.ds(pl.multiple_of(r * 16, 16), 16), pl.ds(n, wide))

    def to_y(u):
        layer, kind, t, i = info[u]
        c_copy(u, 0).wait_recv()
        for j in [*range(1, nz), 0]:
            zz = zrel(j)

            def body(r, n):
                G[t][i, 0, zz, r, n] = (G[t][i, 0, zz, r, n].astype(F32) + C[t][i, 0, zz, r, n].astype(F32)).astype(BF16)

            pieces(t, body)
            y_copy(u, j).start()

    def to_z(u):
        layer, kind, t, i = info[u]
        c_copy(u, 1).wait_recv()
        for k in range(1, nz):
            zz = zrel(k)
            y_copy(u, k).wait_recv()

            def body(r, n):
                G[t][i, 1, zz, r, n] = (
                    G[t][i, 1, zz, r, n].astype(F32) + C[t][i, 1, zz, r, n].astype(F32) + Y[t][i, zz, r, n].astype(F32)
                ).astype(BF16)

            pieces(t, body)
            z_copy(u, k).start()

    pending = [None, None]

    def moments_out(u):
        layer, kind, t, i = info[u]
        return [
            pltpu.make_async_copy(MST[t], nms[kind].at[layer], osem.at[t, 0]),
            pltpu.make_async_copy(VST[t], nvs[kind].at[layer], osem.at[t, 1]),
        ]

    def own_out(u):
        layer, kind, t, i = info[u]
        return pltpu.make_async_copy(G[t].at[i, 1, z], spot(u, me), osem.at[t, 2])

    def send(u, src, d, to, j):
        if to == "z":
            return remote(src, spot(u, d), agz_s.at[u, j], agz_r.at[u, j], z_peers[j])
        if to == "y":
            return remote(src, spot(u, d), agy_s.at[u, j], agy_r.at[u, j], y_peer)
        return remote(src, spot(u, d), agc_s.at[u, j], agc_r.at[u, j], core_peer)

    def finish(u):
        layer, kind, t, i = info[u]
        rows, cols = rows_of(t)
        if pending[t] is not None:
            for copy in moments_out(pending[t]):
                copy.wait()
            own_out(pending[t]).wait()
        loads = [
            pltpu.make_async_copy(ms[kind].at[layer], MST[t], lsem.at[t, 0]),
            pltpu.make_async_copy(vs[kind].at[layer], VST[t], lsem.at[t, 1]),
            pltpu.make_async_copy(ws[kind].at[layer, pl.ds(pl.multiple_of(me * rows, rows), rows), :], WST[t], lsem.at[t, 2]),
        ]
        for copy in loads:
            copy.start()
        y_copy(u, 0).wait_recv()
        for k in range(1, nz):
            z_copy(u, k).wait_recv()
        get_z = pltpu.make_async_copy(zrecv[t].at[i], ZST[t], lsem.at[t, 3])
        get_z.start()
        for copy in [*loads, get_z]:
            copy.wait()

        def body(r, n):
            g = G[t][i, 1, z, r, n].astype(F32) + C[t][i, 1, z, r, n].astype(F32) + Y[t][i, z, r, n].astype(F32)
            for k in range(nz - 1):
                g = g + ZST[t][k, r, n].astype(F32)
            g = g.astype(BF16).astype(F32)
            w = WST[t][r, n].astype(F32)
            m = 0.9 * MST[t][r, n] + 0.1 * g
            v = 0.95 * VST[t][r, n] + 0.05 * g * g
            MST[t][r, n] = m
            VST[t][r, n] = v
            G[t][i, 1, z, r, n] = (w - 0.02 * (m * lax.rsqrt(v + 1e-8) + 0.1 * w)).astype(BF16)

        pieces(t, body)
        mine = G[t].at[i, 1, z]
        for k in range(nz - 1):
            send(u, mine, me, "z", k).start()
        send(u, mine, me, "y", 0).start()
        send(u, mine, me, "core", 0).start()
        for copy in moments_out(u):
            copy.start()
        own_out(u).start()
        pending[t] = u

    def from_z(u):
        for k in range(1, nz):
            d = at_(y, zrel(-k), c)
            send(u, spot(u, d), d, "z", k - 1).wait_recv()
            send(u, spot(u, d), d, "y", k).start()
            send(u, spot(u, d), d, "core", k).start()

    def from_y(u):
        for j in range(nz):
            d = at_(1 - y, zrel(-j), c)
            send(u, spot(u, d), d, "y", j).wait_recv()
            send(u, spot(u, d), d, "core", nz + j).start()

    n = len(units)
    done = {name: 0 for name in "yzfab"}
    stages = {"y": to_y, "z": to_z, "f": finish, "a": from_z, "b": from_y}

    def run(text):
        for s in text:
            stages[s](done[s])
            done[s] += 1

    for u in range(n):
        compute(u, 0)
        if u:
            run("y")
        compute(u, 1)
        if u == 2:
            run("z")
        if u == 3:
            run("z")
        if u == 4:
            run("fz")
    run("y" + "fza" + "fzab" + "fzab" + "fab" + "fab" + "ab" + "b")
    assert all(v == n for v in done.values()), done

    for u in range(n):
        layer, kind, t, i = info[u]
        for h in range(2):
            if last_c[t] == (u, h):
                c_copy(u, h).wait_send()
        for j in range(nz):
            y_copy(u, j).wait_send()
        for k in range(1, nz):
            z_copy(u, k).wait_send()
            send(u, G[t].at[i, 1, z], me, "z", k - 1).wait_send()
        for j in range(nz):
            send(u, G[t].at[i, 1, z], me, "y", j).wait_send()
        for j in range(2 * nz):
            send(u, G[t].at[i, 1, z], me, "core", j).wait_send()
            d = at_(y if j < nz else 1 - y, zrel(-(j % nz)), 1 - c)
            send(u, spot(u, d), d, "core", j).wait_recv()
    for t in range(2):
        for copy in moments_out(pending[t]):
            copy.wait()
        own_out(pending[t]).wait()


def tail(ny, nz, acts, ws, ms, vs):
    units = ((1, 0), (1, 1), (1, 2), (0, 0), (0, 1), (0, 2))
    rg, ff = ms[0].shape[1:]
    rd, dim = ms[2].shape[1:]
    tokens = acts[0][0].shape[0]
    shapes = ((rg, ff), (rd, dim))
    slots = (4, 2)
    n = len(units)
    any_spec = pl.BlockSpec(memory_space=pl.ANY)
    outs = (
        [jax.ShapeDtypeStruct(w.shape, BF16) for w in ws]
        + [jax.ShapeDtypeStruct(m.shape, F32) for m in (*ms, *vs)]
        + [jax.ShapeDtypeStruct((s, nz - 1, *shape), BF16) for s, shape in zip(slots, shapes)]
    )
    scratch = (
        [pltpu.VMEM((s, 2, nz, *shape), BF16) for s, shape in zip(slots, shapes)]
        + [pltpu.VMEM((s, 2, nz, *shape), BF16) for s, shape in zip(slots, shapes)]
        + [pltpu.VMEM((s, nz, *shape), BF16) for s, shape in zip(slots, shapes)]
        + [pltpu.VMEM((nz, *shape), BF16) for shape in shapes]
        + [pltpu.VMEM(shape, F32) for shape in shapes] * 2
        + [pltpu.VMEM(shape, BF16) for shape in shapes]
        + [pltpu.VMEM((nz - 1, *shape), BF16) for shape in shapes]
    )
    half = nz * 2 * max(rg, rd)
    scratch += [
        pltpu.VMEM((tokens, half), BF16),
        pltpu.VMEM((2, 16, half), BF16),
        pltpu.VMEM((2, tokens, CHUNK), BF16),
    ]
    dma = pltpu.SemaphoreType.DMA
    for count in (2, nz, nz - 1, nz - 1, nz, 2 * nz):
        scratch += [dma((n, count)), dma((n, count))]
    scratch += [dma((2,)), dma((2,)), dma((2, 4)), dma((2, 3))]
    flops = 2 * n * tokens * ff * dim
    res = pl.pallas_call(
        functools.partial(tail_kernel, ny, nz, units),
        out_shape=outs,
        in_specs=[any_spec] * (10 + 9),
        out_specs=[any_spec] * len(outs),
        scratch_shapes=scratch,
        compiler_params=pltpu.CompilerParams(collective_id=0, has_side_effects=True, vmem_limit_bytes=67043328),
        cost_estimate=pl.CostEstimate(flops=flops, bytes_accessed=200 << 20, transcendentals=0),
        name="gradients_and_step",
    )(*acts[0], *acts[1], *ws, *ms, *vs)
    return tuple(res[:9])


def solution(mesh):
    nz = 4
    ny = mesh.shape["dp"] // (2 * nz)

    def step(x, dy, *arrays):
        ws, ms, vs = (arrays[i : i + 3] for i in (0, 3, 6))
        acts = chain(x[0], dy[0], *ws)
        return tail(ny, nz, acts, ws, ms, vs)

    mom = P(None, "dp", None)
    return jax.shard_map(
        step,
        mesh=mesh,
        in_specs=(P(("rep", "dp")),) * 2 + (P(),) * 3 + (mom,) * 6,
        out_specs=(P("rep"),) * 3 + (P("rep", "dp", None),) * 6,
        check_vma=False,
    )
```

```python
import functools

import jax
import jax.numpy as jnp
from jax import lax
from jax.experimental import pallas as pl
from jax.experimental.pallas import tpu as pltpu
from jax.sharding import PartitionSpec as P

F32, BF16 = jnp.float32, jnp.bfloat16
KINDS = 3
CHUNK = 256
ORDER = "cccyccyczyAzfzBfPacfycczyaczfcybczaabfbfaabbb"


def matmul(a, w):
    return jnp.dot(a, w, preferred_element_type=F32).astype(BF16)


def matmul_t(a, w):
    return lax.dot_general(a, w, (((1,), (1,)), ((), ())), preferred_element_type=F32).astype(BF16)


def inverse_rms(h):
    wide = h.astype(F32)
    return lax.rsqrt(jnp.mean(wide**2, -1, keepdims=True) + 1e-6)


def forward(h, wg, wu):
    scale = inverse_rms(h)
    a = (h.astype(F32) * scale).astype(BF16)
    gate = jnp.dot(a, wg, preferred_element_type=F32)
    up = jnp.dot(a, wu, preferred_element_type=F32)
    act = (jax.nn.silu(gate) * up).astype(BF16)
    return a, gate, up, act


def through_product(gate, up, dact):
    dact = dact.astype(F32)
    s = jax.nn.sigmoid(gate)
    silu = gate * s
    dgate = dact * up * (s + silu * (1 - s))
    return dgate.astype(BF16), (dact * silu).astype(BF16)


def through_norm(h, da):
    wide, da = h.astype(F32), da.astype(F32)
    scale = inverse_rms(h)
    inner = jnp.sum(da * wide, -1, keepdims=True)
    return (da * scale - wide * (scale**3 * inner / h.shape[-1])).astype(BF16)


def chain(x, dy, wg, wu, wd):
    a0, gate0, up0, act0 = forward(x, wg[0], wu[0])
    h1 = x + matmul(act0, wd[0])
    a1, gate1, up1, act1 = forward(h1, wg[1], wu[1])
    dgate1, dup1 = through_product(gate1, up1, matmul_t(dy, wd[1]))
    return (a0, act0), (a1, dgate1, dup1, act1, dy), (h1, gate0, up0)


def tail_kernel(ny, nz, units, *refs):
    a0, act0, a1, dgate1, dup1, act1, dy, h1, gate0, up0, wg_view, wu_view, dgate1_view, dup1_view = refs[:14]
    refs = refs[14:]
    ws, ms, vs, nws, nms, nvs = (refs[3 * i : 3 * i + 3] for i in range(6))
    zrecv = refs[18:20]
    dgate0, dup0, dh0 = refs[20:23]
    acts = ((a0, dgate0, dup0, act0, dh0), (a1, dgate1, dup1, act1, dy))
    (g0, g1, c0, c1, y0, y1, cs0, cs1, mst0, mst1, vst0, vst1, wst0, wst1, zst0, zst1, at, gu, bt,
     c_s, c_r, y_s, y_r, z_s, z_r, agz_s, agz_r, agy_s, agy_r, agc_s, agc_r, asem, bsem, lsem, osem, psem) = refs[23:]
    G, C, Y, CS = (g0, g1), (c0, c1), (y0, y1), (cs0, cs1)
    MST, VST, WST, ZST = (mst0, mst1), (vst0, vst1), (wst0, wst1), (zst0, zst1)

    me = lax.axis_index("dp")
    c = lax.rem(me, 2)
    z = lax.rem(lax.div(me, 2), nz)
    y = lax.div(me, 2 * nz)

    def at_(yy, zz, cc):
        return (yy * nz + zz) * 2 + cc

    def zrel(k):
        return lax.rem(z + k + nz, nz)

    core_peer = at_(y, z, 1 - c)
    y_peer = at_(1 - y, z, c)
    z_peers = [at_(y, zrel(k), c) for k in range(1, nz)]

    def remote(src, dst, ss, rs, dev):
        return pltpu.make_async_remote_copy(
            src_ref=src, dst_ref=dst, send_sem=ss, recv_sem=rs, device_id={"dp": dev}, device_id_type=pl.DeviceIdType.MESH
        )

    barrier = pltpu.get_barrier_semaphore()
    for dev in [core_peer, y_peer, *z_peers]:
        pl.semaphore_signal(barrier, inc=1, device_id={"dp": dev}, device_id_type=pl.DeviceIdType.MESH)
    pl.semaphore_wait(barrier, 2 + len(z_peers))

    info = []
    seen = [0, 0]
    for layer, kind in units:
        t = int(kind == 2)
        info.append((layer, kind, t, seen[t]))
        seen[t] += 1

    def rows_of(t):
        return G[t].shape[3], G[t].shape[4]

    def c_copy(u, h):
        layer, kind, t, i = info[u]
        return remote(CS[t], C[t].at[i, h], c_s.at[u, h], c_r.at[u, h], core_peer)

    def y_copy(u, j):
        layer, kind, t, i = info[u]
        zz = zrel(j)
        return remote(G[t].at[i, 0, zz], Y[t].at[i, zz], y_s.at[u, j], y_r.at[u, j], y_peer)

    def z_copy(u, k):
        layer, kind, t, i = info[u]
        return remote(G[t].at[i, 1, zrel(k)], zrecv[t].at[i, k - 1], z_s.at[u, k - 1], z_r.at[u, k - 1], z_peers[k - 1])

    def spot(u, d):
        layer, kind, t, i = info[u]
        rows = rows_of(t)[0]
        return nws[kind].at[layer, pl.ds(pl.multiple_of(d * rows, rows), rows), :]

    last_c = [None, None]

    def compute(u, h):
        layer, kind, t, i = info[u]
        a, dgate, dup, act, dh = acts[layer]
        lhs, rhs = ((a, dgate), (a, dup), (act, dh))[kind]
        rows, cols = rows_of(t)
        tokens = lhs.shape[0]
        half = nz * 2 * rows
        yy = y if h else 1 - y
        steps, tiles = tokens // CHUNK, cols // CHUNK

        def get_b(n, slot):
            return pltpu.make_async_copy(rhs.at[:, pl.ds(pl.multiple_of(n * CHUNK, CHUNK), CHUNK)], bt.at[slot], bsem.at[slot, 0])

        whole = pltpu.make_async_copy(lhs.at[:, pl.ds(pl.multiple_of(yy * half, 128), half)], at.at[:, :half], asem.at[0])
        whole.start()
        get_b(0, 0).start()

        whole.wait()
        if last_c[t] is not None:
            c_copy(*last_c[t]).wait_send()

        @pl.loop(0, tiles)
        def _(n):
            slot = lax.rem(n, 2)

            @pl.when(n + 1 < tiles)
            def _():
                get_b(n + 1, 1 - slot).start()

            get_b(n, slot).wait()
            out = lax.dot_general(at[:, :half], bt[slot], (((0,), (0,)), ((), ())), preferred_element_type=F32).astype(BF16)
            out = out.reshape(nz, 2, rows, CHUNK)
            where = pl.ds(pl.multiple_of(n * CHUNK, CHUNK), CHUNK)
            for zz in range(nz):
                first, second = out[zz, 0], out[zz, 1]
                G[t][i, h, zz, :, where] = jnp.where(c == 0, first, second)
                CS[t][zz, :, where] = jnp.where(c == 0, second, first)

        c_copy(u, h).start()
        last_c[t] = (u, h)

    tokens, dim = h1.shape
    tile = 2 * G[0].shape[3]
    block = nz * G[0].shape[3]
    spare = len([1 for layer, kind in units if kind != 2]) // 2

    def across(view, w_view, after):
        matrix = pltpu.make_async_copy(w_view.at[1], G[0].at[pl.ds(spare, 2)], psem.at[0])
        matrix.start()

        def get(s, slot):
            return pltpu.make_async_copy(view.at[pl.ds(s * 2, 2)], CS[0].at[pl.ds(slot * 2, 2)], asem.at[slot])

        if last_c[0] is not None:
            c_copy(*last_c[0]).wait_send()
            last_c[0] = None
        get(0, 0).start()
        if after is not None:
            after.get(0, 0)
        matrix.wait()

        @pl.loop(0, tokens // tile)
        def _(s):
            slot = lax.rem(s, 2)
            rows = pl.ds(pl.multiple_of(s * tile, tile), tile)

            @pl.when(s + 1 < tokens // tile)
            def _():
                get(s + 1, 1 - slot).start()
                if after is not None:
                    after.get(s + 1, 1 - slot)

            get(s, slot).wait()
            lhs = CS[0][pl.ds(slot * 2, 2)].reshape(tile, -1)
            for q in range(4):
                rhs = G[0][spare + q // 2, q % 2].reshape(block, -1)
                part = matmul_t(lhs, rhs)
                cols = slice(q * block, (q + 1) * block)
                if after is None:
                    at[rows, cols] = part
                else:
                    at[rows, cols] = at[rows, cols] + part
            if after is not None:
                after.use(s, slot, rows)

    class Norm:
        @staticmethod
        def copies(s, slot):
            rows = pl.ds(pl.multiple_of(s * tile, tile), tile)
            return [
                pltpu.make_async_copy(src.at[rows, :], G[1].at[1, slot, k, pl.ds(0, tile), :], psem.at[1 + 2 * slot + k])
                for k, src in enumerate((h1, dy))
            ]

        @staticmethod
        def get(s, slot):
            for copy in Norm.copies(s, slot):
                copy.start()

        @staticmethod
        def use(s, slot, rows):
            for copy in Norm.copies(s, slot):
                copy.wait()
            h, by = (G[1][1, slot, k, :tile, :] for k in range(2))
            at[rows, :dim] = by + through_norm(h, at[rows, :dim])

    def dh0_out():
        return pltpu.make_async_copy(at.at[:, :dim], dh0, psem.at[0])

    def into_product():
        part = tokens // 4
        ff = gate0.shape[1]
        piece = CHUNK // 2

        def get_w(n, slot):
            return [
                pltpu.make_async_copy(
                    ws[2].at[0, pl.ds(pl.multiple_of(n * CHUNK + k * piece, piece), piece), :],
                    G[1].at[1, slot, k, pl.ds(0, piece), :],
                    psem.at[1 + 2 * slot + k],
                )
                for k in range(2)
            ]

        def where(n, m):
            return pl.ds(m * part, part), pl.ds(pl.multiple_of(n * CHUNK, CHUNK), CHUNK)

        def get_gu(n, m):
            return [pltpu.make_async_copy(src.at[*where(n, m)], gu.at[m % 2, k], bsem.at[m % 2, k]) for k, src in enumerate((gate0, up0))]

        def put(n, m):
            return [
                pltpu.make_async_copy(bt.at[m % 2, pl.ds(k * part, part), :], dst.at[*where(n, m)], asem.at[2 + 2 * (m % 2) + k])
                for k, dst in enumerate((dgate0, dup0))
            ]

        def each(copies, act):
            for copy in copies:
                act(copy)

        def begin(copy):
            copy.start()

        def end(copy):
            copy.wait()

        each(get_w(0, 0), begin)
        each(get_gu(0, 0), begin)

        @pl.loop(0, ff // CHUNK)
        def _(n):
            slot = lax.rem(n, 2)

            @pl.when(n + 1 < ff // CHUNK)
            def _():
                each(get_w(n + 1, 1 - slot), begin)

            each(get_w(n, slot), end)
            w = jnp.concatenate([G[1][1, slot, k, :piece, :] for k in range(2)], axis=0)
            for m in range(4):
                if m < 3:
                    each(get_gu(n, m + 1), begin)
                else:

                    @pl.when(n + 1 < ff // CHUNK)
                    def _():
                        each(get_gu(n + 1, 0), begin)

                dact = matmul_t(at[m * part : (m + 1) * part, :dim], w)
                each(get_gu(n, m), end)
                if m >= 2:
                    each(put(n, m - 2), end)
                else:

                    @pl.when(n > 0)
                    def _():
                        each(put(n - 1, m + 2), end)

                dgate, dup = through_product(gu[m % 2, 0], gu[m % 2, 1], dact)
                bt[m % 2, :part, :] = dgate
                bt[m % 2, part : 2 * part, :] = dup
                each(put(n, m), begin)

        for m in (2, 3):
            each(put(ff // CHUNK - 1, m), end)

    def pieces(t, body):
        rows, cols = rows_of(t)
        wide = cols // 2 if cols > 2048 else cols

        @pl.loop(0, rows // 16)
        def _(r):
            for n in range(0, cols, wide):
                body(pl.ds(pl.multiple_of(r * 16, 16), 16), pl.ds(n, wide))

    def to_y(u):
        layer, kind, t, i = info[u]
        c_copy(u, 0).wait_recv()
        for j in [*range(1, nz), 0]:
            zz = zrel(j)

            def body(r, n):
                G[t][i, 0, zz, r, n] = (G[t][i, 0, zz, r, n].astype(F32) + C[t][i, 0, zz, r, n].astype(F32)).astype(BF16)

            pieces(t, body)
            y_copy(u, j).start()

    def to_z(u):
        layer, kind, t, i = info[u]
        c_copy(u, 1).wait_recv()
        for k in range(1, nz):
            zz = zrel(k)
            y_copy(u, k).wait_recv()

            def body(r, n):
                G[t][i, 1, zz, r, n] = (
                    G[t][i, 1, zz, r, n].astype(F32) + C[t][i, 1, zz, r, n].astype(F32) + Y[t][i, zz, r, n].astype(F32)
                ).astype(BF16)

            pieces(t, body)
            z_copy(u, k).start()

    pending = [None, None]

    def moments_out(u):
        layer, kind, t, i = info[u]
        return [
            pltpu.make_async_copy(MST[t], nms[kind].at[layer], osem.at[t, 0]),
            pltpu.make_async_copy(VST[t], nvs[kind].at[layer], osem.at[t, 1]),
        ]

    def own_out(u):
        layer, kind, t, i = info[u]
        return pltpu.make_async_copy(G[t].at[i, 1, z], spot(u, me), osem.at[t, 2])

    def send(u, src, d, to, j):
        if to == "z":
            return remote(src, spot(u, d), agz_s.at[u, j], agz_r.at[u, j], z_peers[j])
        if to == "y":
            return remote(src, spot(u, d), agy_s.at[u, j], agy_r.at[u, j], y_peer)
        return remote(src, spot(u, d), agc_s.at[u, j], agc_r.at[u, j], core_peer)

    def finish(u):
        layer, kind, t, i = info[u]
        rows, cols = rows_of(t)
        if pending[t] is not None:
            for copy in moments_out(pending[t]):
                copy.wait()
            own_out(pending[t]).wait()
        loads = [
            pltpu.make_async_copy(ms[kind].at[layer], MST[t], lsem.at[t, 0]),
            pltpu.make_async_copy(vs[kind].at[layer], VST[t], lsem.at[t, 1]),
            pltpu.make_async_copy(ws[kind].at[layer, pl.ds(pl.multiple_of(me * rows, rows), rows), :], WST[t], lsem.at[t, 2]),
        ]
        for copy in loads:
            copy.start()
        y_copy(u, 0).wait_recv()
        for k in range(1, nz):
            z_copy(u, k).wait_recv()
        get_z = pltpu.make_async_copy(zrecv[t].at[i], ZST[t], lsem.at[t, 3])
        get_z.start()
        for copy in [*loads, get_z]:
            copy.wait()

        def body(r, n):
            g = G[t][i, 1, z, r, n].astype(F32) + C[t][i, 1, z, r, n].astype(F32) + Y[t][i, z, r, n].astype(F32)
            for k in range(nz - 1):
                g = g + ZST[t][k, r, n].astype(F32)
            g = g.astype(BF16).astype(F32)
            w = WST[t][r, n].astype(F32)
            m = 0.9 * MST[t][r, n] + 0.1 * g
            v = 0.95 * VST[t][r, n] + 0.05 * g * g
            MST[t][r, n] = m
            VST[t][r, n] = v
            G[t][i, 1, z, r, n] = (w - 0.02 * (m * lax.rsqrt(v + 1e-8) + 0.1 * w)).astype(BF16)

        pieces(t, body)
        mine = G[t].at[i, 1, z]
        for k in range(nz - 1):
            send(u, mine, me, "z", k).start()
        send(u, mine, me, "y", 0).start()
        send(u, mine, me, "core", 0).start()
        for copy in moments_out(u):
            copy.start()
        own_out(u).start()
        pending[t] = u

    def from_z(u):
        for k in range(1, nz):
            d = at_(y, zrel(-k), c)
            send(u, spot(u, d), d, "z", k - 1).wait_recv()
            send(u, spot(u, d), d, "y", k).start()
            send(u, spot(u, d), d, "core", k).start()

    def from_y(u):
        for j in range(nz):
            d = at_(1 - y, zrel(-j), c)
            send(u, spot(u, d), d, "y", j).wait_recv()
            send(u, spot(u, d), d, "core", nz + j).start()

    n = len(units)
    done = {name: 0 for name in "yzfab"}
    stages = {"y": to_y, "z": to_z, "f": finish, "a": from_z, "b": from_y}

    def run(text):
        for s in text:
            stages[s](done[s])
            done[s] += 1

    halves = 0
    for step in ORDER:
        if step == "c":
            compute(*divmod(halves, 2))
            halves += 1
        elif step == "A":
            across(dgate1_view, wg_view, None)
        elif step == "B":
            across(dup1_view, wu_view, Norm)
            dh0_out().start()
        elif step == "P":
            into_product()
            dh0_out().wait()
        else:
            run(step)
    assert all(v == n for v in done.values()), done

    for u in range(n):
        layer, kind, t, i = info[u]
        for h in range(2):
            if last_c[t] == (u, h):
                c_copy(u, h).wait_send()
        for j in range(nz):
            y_copy(u, j).wait_send()
        for k in range(1, nz):
            z_copy(u, k).wait_send()
            send(u, G[t].at[i, 1, z], me, "z", k - 1).wait_send()
        for j in range(nz):
            send(u, G[t].at[i, 1, z], me, "y", j).wait_send()
        for j in range(2 * nz):
            send(u, G[t].at[i, 1, z], me, "core", j).wait_send()
            d = at_(y if j < nz else 1 - y, zrel(-(j % nz)), 1 - c)
            send(u, spot(u, d), d, "core", j).wait_recv()
    for t in range(2):
        for copy in moments_out(pending[t]):
            copy.wait()
        own_out(pending[t]).wait()


def tail(ny, nz, acts0, acts1, rest, ws, ms, vs):
    units = ((1, 0), (1, 1), (1, 2), (0, 0), (0, 1), (0, 2))
    rg, ff = ms[0].shape[1:]
    rd, dim = ms[2].shape[1:]
    tokens = acts1[0].shape[0]
    shapes = ((rg, ff), (rd, dim))
    slots = (4, 2)
    n = len(units)
    any_spec = pl.BlockSpec(memory_space=pl.ANY)
    outs = (
        [jax.ShapeDtypeStruct(w.shape, BF16) for w in ws]
        + [jax.ShapeDtypeStruct(m.shape, F32) for m in (*ms, *vs)]
        + [jax.ShapeDtypeStruct((s, nz - 1, *shape), BF16) for s, shape in zip(slots, shapes)]
        + [jax.ShapeDtypeStruct(s, BF16) for s in ((tokens, ff), (tokens, ff), (tokens, dim))]
    )
    scratch = (
        [pltpu.VMEM((s, 2, nz, *shape), BF16) for s, shape in zip(slots, shapes)]
        + [pltpu.VMEM((s, 2, nz, *shape), BF16) for s, shape in zip(slots, shapes)]
        + [pltpu.VMEM((s, nz, *shape), BF16) for s, shape in zip(slots, shapes)]
        + [pltpu.VMEM((nz, *shape), BF16) for shape in shapes]
        + [pltpu.VMEM(shape, F32) for shape in shapes] * 2
        + [pltpu.VMEM(shape, BF16) for shape in shapes]
        + [pltpu.VMEM((nz - 1, *shape), BF16) for shape in shapes]
    )
    half = nz * 2 * max(rg, rd)
    scratch += [
        pltpu.VMEM((tokens, half), BF16),
        pltpu.VMEM((2, 2, tokens // 4, CHUNK), F32),
        pltpu.VMEM((2, tokens, CHUNK), BF16),
    ]
    dma = pltpu.SemaphoreType.DMA
    for count in (2, nz, nz - 1, nz - 1, nz, 2 * nz):
        scratch += [dma((n, count)), dma((n, count))]
    scratch += [dma((6,)), dma((2, 2)), dma((2, 4)), dma((2, 3)), dma((5,))]
    flops = 3 * n * tokens * ff * dim
    res = pl.pallas_call(
        functools.partial(tail_kernel, ny, nz, units),
        out_shape=outs,
        in_specs=[any_spec] * (14 + 9),
        out_specs=[any_spec] * len(outs),
        scratch_shapes=scratch,
        compiler_params=pltpu.CompilerParams(collective_id=0, has_side_effects=True, vmem_limit_bytes=67043328),
        cost_estimate=pl.CostEstimate(flops=flops, bytes_accessed=200 << 20, transcendentals=0),
        name="gradients_and_step",
    )(
        *acts0,
        *acts1,
        *rest,
        *(w.reshape(-1, 2, 2, nz, rg, ff) for w in ws[:2]),
        *(t.reshape(-1, rg, ff) for t in acts1[1:3]),
        *ws,
        *ms,
        *vs,
    )
    return tuple(res[:9])


def solution(mesh):
    nz = 4
    ny = mesh.shape["dp"] // (2 * nz)

    def step(x, dy, *arrays):
        ws, ms, vs = (arrays[i : i + 3] for i in (0, 3, 6))
        acts = chain(x[0], dy[0], *ws)
        return tail(ny, nz, *acts, ws, ms, vs)

    mom = P(None, "dp", None)
    return jax.shard_map(
        step,
        mesh=mesh,
        in_specs=(P(("rep", "dp")),) * 2 + (P(),) * 3 + (mom,) * 6,
        out_specs=(P("rep"),) * 3 + (P("rep", "dp", None),) * 6,
        check_vma=False,
    )
```
